32 devices in a mesh: depth: 8 (over z, y), lat: 4 (over x, core).
Axes of the slice: x: 2, y: 2, z: 4, core: 2. Of those that a mesh axis runs over, the one named last changes fastest.
Arguments:
- density: bfloat16 [8, 16, 512, 2048], P('depth', None, None, 'lat'), may hold values from 0 to 1
- occupancy: int32 [8, 4, 16], P('depth', None, 'lat'), may hold values from 0 to 1, as said below
- shear_offsets: int32 [8, 16], P('depth'), may hold values from 0 to 127, as said below
- frac_lateral: float32 [8, 16], P('depth'), may hold values from 0.05 to 0.95
- frac_vertical: float32 [8, 16], P('depth'), may hold values from 0.05 to 0.95
- extinction: float32 [8, 16], P('depth'), may hold values from 2 to 32
- slab_gain: float32 [8], P('depth'), may hold values from 0.05 to 1
- view_rank: int32 [8], replicated, may hold values from 0 to 7, as said below
Outputs:
- image_color: float32 [512, 2048], P('depth', 'lat')
- image_alpha: float32 [512, 2048], P('depth', 'lat')
The draws below stay inside these ranges and needn't reach their ends.
Inputs may be any that keep to these rules, and one draw needn't show every extreme that they name: `occupancy`: A block is 1 if occupied; the share of occupied blocks differs from slab to slab. `shear_offsets`: some slice has the offset 128 - 1. `view_rank`: A permutation of the slabs in which every aligned group of a power of two of slabs holds consecutive ranks.
All inputs are finite; a program needn't handle non-finite values.
Results may differ from the reference program's by a relative error of at most 0.00077.
Values may be sent and summed in bfloat16 or wider, within the bound.
A program may use at most 128 MiB of HBM per device.

```python
import math
import jax
import jax.numpy as jnp
from jax import lax

SL = 16
ROWS = 512
WID = 512
SHIFT = 128
BLK = 128
SLABS = 8
NBR = 4
IMGW = 2048
N_LAT = 4


def draw_occupancy(key, part):
    level_key = jax.random.fold_in(key, 11)
    cell_key = jax.random.fold_in(key, 12)
    fill_level = jax.random.randint(level_key, (SLABS, 1, 1), 1, 9)
    cells = jax.random.randint(cell_key, (SLABS, NBR, IMGW // BLK), 0, 8)
    return (cells < fill_level).astype(jnp.int32)


def draw_shear_offsets(key, part):
    value_key = jax.random.fold_in(key, 21)
    place_key = jax.random.fold_in(key, 22)
    values = jax.random.randint(value_key, (SLABS * SL,), 0, SHIFT)
    where_max = jax.random.randint(place_key, (), 0, SLABS * SL)
    values = values.at[where_max].set(SHIFT - 1)
    return values.reshape(SLABS, SL).astype(jnp.int32)


def draw_view_rank(key, part):
    flip_key = jax.random.fold_in(key, 31)
    level_count = SLABS.bit_length() - 1
    flip_table = jax.random.randint(flip_key, (level_count, SLABS), 0, 2).astype(jnp.int32)
    slab_index = jnp.arange(SLABS, dtype=jnp.int32)
    ranks = jnp.zeros((SLABS,), jnp.int32)
    for level in range(level_count):
        node = jnp.right_shift(slab_index, level + 1)
        flip_bit = flip_table[level][node]
        own_bit = jnp.bitwise_and(jnp.right_shift(slab_index, level), 1)
        ranks = ranks + jnp.left_shift(jnp.bitwise_xor(own_bit, flip_bit), level)
    return ranks.astype(jnp.int32)


def level_of(rng, shape, pieces, low, high):
    def one(position, shards_of):
        steps = jax.random.uniform(jax.random.fold_in(jax.random.fold_in(rng, 6), position), (shards_of,), jnp.float32, low / len(pieces), high / len(pieces))
        return jnp.repeat(jnp.exp(steps), shape[position] // shards_of).reshape((-1,) + (1,) * (len(shape) - position - 1))

    level = one(*pieces[0])
    for cut in pieces[1:]:
        level = level * one(*cut)
    return level


def setup_inputs(seed: int = 0) -> dict:
    arg_keys = jax.random.split(jax.random.key(seed), 9)
    density = jnp.clip(1.0 * jax.random.uniform(arg_keys[0], (SLABS, SL, ROWS, IMGW), jnp.float32) ** level_of(arg_keys[0], (SLABS, SL, ROWS, IMGW), ((0, 8), (3, 4)), -0.2, 0.2), 0.0, 1.0).astype(jnp.bfloat16)
    occupancy = draw_occupancy(jax.random.fold_in(arg_keys[8], 71), 0)
    shear_offsets = draw_shear_offsets(jax.random.fold_in(arg_keys[8], 71), 0)
    frac_lateral = jnp.clip(0.05 + 0.9 * jax.random.uniform(arg_keys[3], (SLABS, SL), jnp.float32) ** level_of(arg_keys[3], (SLABS, SL), ((0, 8),), -0.2, 0.2), 0.05, 0.95)
    frac_vertical = jnp.clip(0.05 + 0.9 * jax.random.uniform(arg_keys[4], (SLABS, SL), jnp.float32) ** level_of(arg_keys[4], (SLABS, SL), ((0, 8),), -0.2, 0.2), 0.05, 0.95)
    extinction = jnp.clip(jnp.exp(math.log(32.0) - 2.7725887 * jax.random.uniform(arg_keys[5], (SLABS, SL), jnp.float32) ** level_of(arg_keys[5], (SLABS, SL), ((0, 8),), -0.2, 0.2)), 2.0, 32.0)
    slab_gain = jnp.clip(jnp.exp(math.log(1.0) - 2.9957323 * jax.random.uniform(arg_keys[6], (SLABS,), jnp.float32) ** level_of(arg_keys[6], (SLABS,), ((0, 8),), -0.2, 0.2)), 0.05, 1.0)
    view_rank = draw_view_rank(jax.random.fold_in(arg_keys[8], 71), 0)
    return {"density": density, "occupancy": occupancy, "shear_offsets": shear_offsets, "frac_lateral": frac_lateral, "frac_vertical": frac_vertical, "extinction": extinction, "slab_gain": slab_gain, "view_rank": view_rank}


def lateral_weights(offsets, fraction, in_count, out_count):
    source = jnp.arange(in_count, dtype=jnp.int32)[None, :, None]
    target = jnp.arange(out_count, dtype=jnp.int32)[None, None, :]
    shifted = target - offsets[:, None, None]
    first_term = jnp.where(shifted == source, (1.0 - fraction)[:, None, None], 0.0)
    second = jnp.where(shifted - 1 == source, fraction[:, None, None], 0.0)
    return (first_term + second).astype(jnp.bfloat16)


def vertical_weights(fraction, row_count):
    target = jnp.arange(row_count, dtype=jnp.int32)[None, :, None]
    source = jnp.arange(row_count, dtype=jnp.int32)[None, None, :]
    first_term = jnp.where(target == source, (1.0 - fraction)[:, None, None], 0.0)
    second = jnp.where(target - 1 == source, fraction[:, None, None], 0.0)
    return (first_term + second).astype(jnp.bfloat16)


def shade_slices(density_sum, extinction, gain, slice_total):
    row_above = jnp.pad(density_sum, ((0, 0), (1, 0), (0, 0)))[:, :-1, :]
    shading = 0.3 + 0.7 * jax.nn.sigmoid(4.0 * (density_sum - row_above))
    opacity = 1.0 - jnp.exp(-extinction[:, None, None] * density_sum / slice_total)
    emission = opacity * shading * gain
    through = jnp.cumprod(1.0 - opacity, axis=0)
    before = jnp.concatenate([jnp.ones_like(through[:1]), through[:-1]], axis=0)
    return jnp.sum(emission * before, axis=0), 1.0 - through[-1]


def reference(density, occupancy, shear_offsets, frac_lateral, frac_vertical, extinction, slab_gain, view_rank):
    def one_slab(slab_items):
        slab_voxels, occ_blocks, offsets, lateral_frac, vertical_frac, slab_ext, gain = slab_items
        block_mask = jnp.repeat(jnp.repeat(occ_blocks, BLK, axis=0), BLK, axis=1).astype(jnp.bfloat16)
        masked = (slab_voxels * block_mask[None]).reshape(SL, ROWS, N_LAT, WID)
        lateral_matrix = lateral_weights(offsets, lateral_frac, WID, WID + SHIFT)
        across = jnp.einsum('srbw,swq->srbq', masked.astype(jnp.float32), lateral_matrix.astype(jnp.float32)).astype(jnp.bfloat16)
        vertical_matrix = vertical_weights(vertical_frac, ROWS)
        resampled = jnp.einsum('sij,sjbq->sibq', vertical_matrix.astype(jnp.float32), across.astype(jnp.float32)).astype(jnp.bfloat16)
        local_part = resampled[..., :WID].astype(jnp.float32)
        edge_spill = resampled[..., WID:].astype(jnp.float32)
        incoming = jnp.concatenate([jnp.zeros_like(edge_spill[:, :, :1]), edge_spill[:, :, :-1]], axis=2)
        incoming = jnp.pad(incoming, ((0, 0), (0, 0), (0, 0), (0, WID - SHIFT)))
        density_sum = (local_part + incoming).reshape(SL, ROWS, N_LAT * WID)
        return shade_slices(density_sum, slab_ext, gain, SLABS * SL)

    slab_colors, slab_alphas = lax.map(one_slab, (density, occupancy, shear_offsets, frac_lateral, frac_vertical, extinction, slab_gain))
    view_order = jnp.argsort(view_rank)
    slab_colors = slab_colors[view_order]
    slab_alphas = slab_alphas[view_order]

    def composite(running, slab_pair):
        run_color, run_alpha = running
        next_color, next_alpha = slab_pair
        return (run_color + (1.0 - run_alpha) * next_color, run_alpha + (1.0 - run_alpha) * next_alpha), None

    start = (jnp.zeros(slab_colors.shape[1:], slab_colors.dtype), jnp.zeros(slab_alphas.shape[1:], slab_alphas.dtype))
    (image_color, image_alpha), _ = lax.scan(composite, start, (slab_colors, slab_alphas))
    return image_color, image_alpha
```

```python
import functools
import math

import jax
import jax.numpy as jnp
from jax import lax
from jax.experimental import pallas as pl
from jax.experimental.pallas import tpu as pltpu
from jax.sharding import PartitionSpec as P

SHIFT = 128
BLK = 128
HALO = 16


def rounded(x):
    return x.astype(jnp.bfloat16).astype(jnp.float32)


def build_lateral(lmat, off, prm, slices):
    source = lax.broadcasted_iota(jnp.int32, (2 * SHIFT, SHIFT), 0)
    target = lax.broadcasted_iota(jnp.int32, (2 * SHIFT, SHIFT), 1)
    lag = target + SHIFT - source
    for s in range(slices):
        first = jnp.where(lag == off[0, s], prm[0, s], 0.0)
        second = jnp.where(lag - 1 == off[0, s], prm[1, s], 0.0)
        lmat[s] = (first + second).astype(jnp.bfloat16)


def march(r, left, right, left_occ, left_halo, right_occ, right_halo, lmat, prm, slices):
    row = pl.multiple_of(r * BLK, BLK)
    above = pl.multiple_of(jnp.maximum(r * BLK - HALO, 0), HALO)

    def scaled(ref, s, start, count, by):
        return ref[s, pl.ds(start, count), :] * jnp.full((count, SHIFT), by).astype(jnp.bfloat16)

    through = jnp.ones((BLK, SHIFT), jnp.float32)
    color = jnp.zeros((BLK, SHIFT), jnp.float32)
    for s in range(slices):
        top = jnp.concatenate(
            [scaled(left, s, above, HALO, left_halo), scaled(right, s, above, HALO, right_halo)], 1
        )
        body = jnp.concatenate(
            [scaled(left, s, row, BLK, left_occ), scaled(right, s, row, BLK, right_occ)], 1
        )
        voxels = jnp.concatenate([top, body], 0)
        across = rounded(jnp.dot(voxels, lmat[s], preferred_element_type=jnp.float32))
        field = rounded(prm[2, s] * across + prm[3, s] * pltpu.roll(across, 1, 0))
        slope = (field - pltpu.roll(field, 1, 0))[HALO:]
        after = through * jnp.exp2(prm[4, s] * field[HALO:])
        color = color + (through - after) * jnp.tanh(slope)
        through = after
    return color, through


def finish(color, through, gain):
    alpha = 1.0 - through
    return gain * (0.35 * color + 0.65 * alpha), alpha


def main_kernel(slices, left, right, occ, off, prm, gain, color_out, alpha_out, lmat):
    t, r = pl.program_id(0), pl.program_id(1)

    @pl.when((t == 0) & (r == 0))
    def _():
        build_lateral(lmat, off, prm, slices)

    up = jnp.maximum(r - 1, 0)
    inside = jnp.where(r > 0, 1.0, 0.0)
    color, through = march(
        r, left, right, occ[r, t], occ[up, t] * inside, occ[r, t + 1], occ[up, t + 1] * inside,
        lmat, prm, slices,
    )
    color_out[...], alpha_out[...] = finish(color, through, gain[0])


def edge_kernel(slices, left, right, occ, off, prm, gain, color_out, alpha_out, lmat):
    r = pl.program_id(0)

    @pl.when(r == 0)
    def _():
        build_lateral(lmat, off, prm, slices)

    up = jnp.maximum(r - 1, 0)
    inside = jnp.where(r > 0, 1.0, 0.0)
    color, through = march(
        r, left, right, 1.0, inside, occ[r, 0], occ[up, 0] * inside, lmat, prm, slices
    )
    color_out[...], alpha_out[...] = finish(color, through, gain[0])


def from_behind(value, axis, steps):
    count = lax.axis_size(axis)
    leading, last = (max(0, -steps), min(count, count - steps))
    return lax.ppermute(value, axis, [(source, source + steps) for source in range(leading, last)])


def partner(value, axis, bit):
    mask = 2**bit
    pairs = [(source, source ^ mask) for source in range(lax.axis_size(axis))]
    return lax.ppermute(value, axis, pairs)


def composite(front_color, front_alpha, back_color, back_alpha):
    return (
        front_color + (1.0 - front_alpha) * back_color,
        front_alpha + (1.0 - front_alpha) * back_alpha,
    )


def encode(x):
    return jnp.round(x * 65535.0 - 32768.0).astype(jnp.int16)


def decode(x):
    return (x.astype(jnp.float32) + 32768.0) * (1.0 / 65535.0)


def shards(
    density, occupancy, shear_offsets, frac_lateral, frac_vertical, extinction, slab_gain, view_rank
):
    voxels = density[0]
    slices, rows, cols = voxels.shape
    row_blocks, col_blocks = rows // BLK, cols // SHIFT
    occ = occupancy[0].astype(jnp.float32)
    slice_total = lax.axis_size("depth") * slices
    prm = jnp.stack(
        [
            1.0 - frac_lateral[0],
            frac_lateral[0],
            2.0 * lax.reduce_precision(1.0 - frac_vertical[0], 8, 7),
            2.0 * lax.reduce_precision(frac_vertical[0], 8, 7),
            extinction[0] * (-0.5 * math.log2(math.e) / slice_total),
        ]
    )
    edge_mask = jnp.repeat(occ[:, -1], BLK).astype(jnp.bfloat16)
    edge = from_behind(voxels[:, :, cols - SHIFT :] * edge_mask[None, :, None], "lat", 1)
    smem = pl.BlockSpec(memory_space=pltpu.SMEM)
    tile = (slices, rows, SHIFT)
    scratch = [pltpu.VMEM((slices, 2 * SHIFT, SHIFT), jnp.bfloat16)]
    main_color, main_alpha = pl.pallas_call(
        functools.partial(main_kernel, slices),
        grid=(col_blocks - 1, row_blocks),
        in_specs=[
            pl.BlockSpec(tile, lambda t, r: (0, 0, t)),
            pl.BlockSpec(tile, lambda t, r: (0, 0, t + 1)),
            smem, smem, smem, smem,
        ],
        out_specs=[pl.BlockSpec((BLK, SHIFT), lambda t, r: (r, t))] * 2,
        out_shape=[jax.ShapeDtypeStruct((rows, cols - SHIFT), jnp.float32)] * 2,
        scratch_shapes=scratch,
        cost_estimate=pl.CostEstimate(
            flops=8 * 10**9, bytes_accessed=16 * 2**20, transcendentals=8 * 10**6
        ),
    )(voxels, voxels, occ, shear_offsets, prm, slab_gain)
    edge_color, edge_alpha = pl.pallas_call(
        functools.partial(edge_kernel, slices),
        grid=(row_blocks,),
        in_specs=[
            pl.BlockSpec(tile, lambda r: (0, 0, 0)),
            pl.BlockSpec(tile, lambda r: (0, 0, 0)),
            smem, smem, smem, smem,
        ],
        out_specs=[pl.BlockSpec((BLK, SHIFT), lambda r: (r, 0))] * 2,
        out_shape=[jax.ShapeDtypeStruct((rows, SHIFT), jnp.float32)] * 2,
        scratch_shapes=scratch,
        cost_estimate=pl.CostEstimate(
            flops=3 * 10**9, bytes_accessed=4 * 2**20, transcendentals=2 * 10**6
        ),
    )(edge, voxels, occ, shear_offsets, prm, slab_gain)
    image_color = jnp.concatenate([edge_color, main_color], 1)
    image_alpha = jnp.concatenate([edge_alpha, main_alpha], 1)

    device_index = lax.axis_index("depth")
    group_size = lax.axis_size("depth")
    piece_rows = rows // group_size
    my_rank = view_rank[device_index]
    held = jnp.stack([image_color, image_alpha]).reshape(2, group_size, piece_rows, cols)
    for bit_level in range(group_size.bit_length() - 1):
        device_bit = device_index >> bit_level & 1
        paired = held.reshape(2, held.shape[1] // 2, 2, piece_rows, cols)
        keep = lax.dynamic_index_in_dim(paired, device_bit, 2, keepdims=False)
        send = lax.dynamic_index_in_dim(paired, 1 - device_bit, 2, keepdims=False)
        other = decode(partner(encode(send), "depth", bit_level))
        in_front = my_rank >> bit_level & 1 == 0
        front = jnp.where(in_front, keep, other)
        back = jnp.where(in_front, other, keep)
        held = jnp.stack(composite(front[0], front[1], back[0], back[1]))
    return held[0].reshape(piece_rows, cols), held[1].reshape(piece_rows, cols)


def solution(mesh):
    placed = (
        P("depth", None, None, "lat"),
        P("depth", None, "lat"),
        P("depth", None),
        P("depth", None),
        P("depth", None),
        P("depth", None),
        P("depth"),
        P(),
    )
    return jax.shard_map(
        shards,
        mesh=mesh,
        in_specs=placed,
        out_specs=(P("depth", "lat"), P("depth", "lat")),
        check_vma=False,
    )
```

```python
import functools
import math

import jax
import jax.numpy as jnp
from jax import lax
from jax.experimental import pallas as pl
from jax.experimental.pallas import tpu as pltpu
from jax.sharding import PartitionSpec as P

SHIFT = 128
BLK = 128
HALO = 16


def rounded(x):
    return x.astype(jnp.bfloat16).astype(jnp.float32)


def build_lateral(lmat, off, prm, slices):
    source = lax.broadcasted_iota(jnp.int32, (2 * SHIFT, SHIFT), 0)
    target = lax.broadcasted_iota(jnp.int32, (2 * SHIFT, SHIFT), 1)
    lag = target + SHIFT - source
    for s in range(slices):
        first = jnp.where(lag == off[0, s], prm[0, s], 0.0)
        second = jnp.where(lag - 1 == off[0, s], prm[1, s], 0.0)
        lmat[s] = (first + second).astype(jnp.bfloat16)


def march(r, left, right, masks, lmat, prm, slices):
    row = pl.multiple_of(r * BLK, BLK)
    above = pl.multiple_of(jnp.maximum(r * BLK - HALO, 0), HALO)
    left_occ, left_halo, right_occ, right_halo = [
        jnp.broadcast_to(mask, (HALO, SHIFT)).astype(jnp.bfloat16) for mask in masks
    ]

    def scaled(read, s, start, count, by):
        return read(s, start, count) * jnp.concatenate([by] * (count // HALO), 0)

    through = jnp.ones((BLK, SHIFT), jnp.float32)
    color = jnp.zeros((BLK, SHIFT), jnp.float32)
    for s in range(slices):
        top = jnp.concatenate(
            [scaled(left, s, above, HALO, left_halo), scaled(right, s, above, HALO, right_halo)], 1
        )
        body = jnp.concatenate(
            [scaled(left, s, row, BLK, left_occ), scaled(right, s, row, BLK, right_occ)], 1
        )
        voxels = jnp.concatenate([top, body], 0)
        across = rounded(jnp.dot(voxels, lmat[s], preferred_element_type=jnp.float32))
        field = rounded(prm[2, s] * across + prm[3, s] * pltpu.roll(across, 1, 0))
        slope = (field - pltpu.roll(field, 1, 0))[HALO:]
        after = through * jnp.exp2(prm[4, s] * field[HALO:])
        color = color + (through - after) * jnp.tanh(slope)
        through = after
    return color, through


def finish(color, through, gain):
    alpha = 1.0 - through
    return gain * (0.35 * color + 0.65 * alpha), alpha


def encode(x):
    return jnp.floor(x * 65535.0 - 32767.5).astype(jnp.int32).astype(jnp.int16)


def decode(x):
    return (x.astype(jnp.int32).astype(jnp.float32) + 32768.0) * (1.0 / 65535.0)


def over(in_front, keep, other):
    keep_color, keep_alpha = keep
    other_color, other_alpha = other
    front_color = jnp.where(in_front, keep_color, other_color)
    front_alpha = jnp.where(in_front, keep_alpha, other_alpha)
    back_color = jnp.where(in_front, other_color, keep_color)
    back_alpha = jnp.where(in_front, other_alpha, keep_alpha)
    return (
        front_color + (1.0 - front_alpha) * back_color,
        front_alpha + (1.0 - front_alpha) * back_alpha,
    )


def render_kernel(
    dims,
    density, occ_edge, occ, off, prm, gain, view_rank,
    color_out, alpha_out,
    voxels, edge, occ_left, lmat, held, first_out, first_in, later_out, later_in,
    load_sem, edge_send, edge_recv, occ_send, occ_recv, first_send, first_recv,
    later_send, later_recv,
):
    slices, rows, cols, group, lanes = dims
    row_blocks, col_blocks = rows // BLK, cols // SHIFT
    piece = rows // group
    pairs = BLK // (2 * piece)
    levels = group.bit_length() - 1
    me, lat = lax.axis_index("depth"), lax.axis_index("lat")
    has_left, has_right = lat > 0, lat < lanes - 1
    my_rank = view_rank[me]

    def depth_id(level):
        return {"depth": me ^ (1 << level), "lat": lat}

    def bit(level):
        return (me >> level) & 1

    def in_front(level):
        return ((my_rank >> level) & 1) == 0

    barrier = pltpu.get_barrier_semaphore()
    for level in range(levels):
        pl.semaphore_signal(
            barrier, inc=1, device_id=depth_id(level), device_id_type=pl.DeviceIdType.MESH
        )

    right_id = {"depth": me, "lat": jnp.minimum(lat + 1, lanes - 1)}
    left_id = {"depth": me, "lat": jnp.maximum(lat - 1, 0)}

    @pl.when(has_left)
    def _():
        pl.semaphore_signal(barrier, inc=1, device_id=left_id, device_id_type=pl.DeviceIdType.MESH)

    @pl.when(has_right)
    def _():
        pl.semaphore_signal(barrier, inc=1, device_id=right_id, device_id_type=pl.DeviceIdType.MESH)

    def load(r):
        span = pl.ds(pl.multiple_of(r * BLK, BLK), BLK)
        return pltpu.make_async_copy(
            density.at[:, span, :], voxels.at[:, span, :], load_sem.at[r]
        )

    def edge_copy(r):
        span = pl.ds(pl.multiple_of(r * BLK, BLK), BLK)
        return pltpu.make_async_remote_copy(
            src_ref=density.at[:, span, pl.ds(cols - SHIFT, SHIFT)],
            dst_ref=edge.at[:, span, :],
            send_sem=edge_send.at[r],
            recv_sem=edge_recv.at[r],
            device_id=right_id,
            device_id_type=pl.DeviceIdType.MESH,
        )

    occ_copy = pltpu.make_async_remote_copy(
        src_ref=occ_edge,
        dst_ref=occ_left,
        send_sem=occ_send,
        recv_sem=occ_recv,
        device_id=right_id,
        device_id_type=pl.DeviceIdType.MESH,
    )

    def first_copy(r):
        return pltpu.make_async_remote_copy(
            src_ref=first_out.at[r],
            dst_ref=first_in.at[r],
            send_sem=first_send.at[r],
            recv_sem=first_recv.at[r],
            device_id=depth_id(0),
            device_id_type=pl.DeviceIdType.MESH,
        )

    for r in range(row_blocks):
        load(r).start()

    @pl.when(jnp.logical_not(has_left))
    def _():
        edge[...] = jnp.zeros_like(edge)
        occ_left[...] = jnp.zeros_like(occ_left)

    build_lateral(lmat, off, prm, slices)

    wanted = levels + has_left.astype(jnp.int32) + has_right.astype(jnp.int32)
    pl.semaphore_wait(barrier, wanted)

    @pl.when(has_right)
    def _():
        occ_copy.start()
        for r in range(row_blocks):
            edge_copy(r).start()

    odd = bit(0) == 1
    zero = jnp.zeros((1, SHIFT), jnp.float32)

    def read_voxels(t):
        def read(s, start, count):
            return voxels[s, pl.ds(start, count), pl.ds(pl.multiple_of(t * SHIFT, SHIFT), SHIFT)]
        return read

    def read_edge(s, start, count):
        return edge[s, pl.ds(start, count), :]

    def tile(r, t, left, left_mask, left_halo):
        up = jnp.maximum(r - 1, 0)
        inside = jnp.where(r > 0, 1.0, 0.0)
        masks = (left_mask, left_halo * inside, zero + occ[r, t], zero + occ[up, t] * inside)
        result = finish(*march(r, left, read_voxels(t), masks, lmat, prm, slices), gain[0])
        lane = pl.ds(pl.multiple_of(t * SHIFT, SHIFT), SHIFT)
        for channel in range(2):
            for k in range(pairs):
                low = result[channel][2 * k * piece : (2 * k + 1) * piece]
                high = result[channel][(2 * k + 1) * piece : (2 * k + 2) * piece]
                held[channel, r * pairs + k, :, lane] = jnp.where(odd, high, low)
                first_out[r, channel, k, :, lane] = encode(jnp.where(odd, low, high))

    def first_merge(r):
        first_copy(r).wait()
        for k in range(pairs):
            keep = held[0, r * pairs + k], held[1, r * pairs + k]
            other = decode(first_in[r, 0, k]), decode(first_in[r, 1, k])
            held[0, r * pairs + k], held[1, r * pairs + k] = over(in_front(0), keep, other)

    def row_step(r, carry):
        load(r).wait()

        def col_step(t, inner):
            up = jnp.maximum(r - 1, 0)
            tile(r, t, read_voxels(t - 1), zero + occ[r, t - 1], zero + occ[up, t - 1])
            return inner

        lax.fori_loop(1, col_blocks, col_step, 0)

        @pl.when(has_left & (r == 0))
        def _():
            occ_copy.wait_recv()

        @pl.when(has_left)
        def _():
            edge_copy(r).wait_recv()

        up = jnp.maximum(r - 1, 0)
        tile(r, 0, read_edge, occ_left[pl.ds(r, 1), :], occ_left[pl.ds(up, 1), :])
        first_copy(r).start()

        @pl.when(r > 0)
        def _():
            first_merge(r - 1)

        return carry

    lax.fori_loop(0, row_blocks, row_step, 0)

    @pl.when(has_right)
    def _():
        occ_copy.wait_send()
        for r in range(row_blocks):
            edge_copy(r).wait_send()

    first_merge(row_blocks - 1)

    slot = 0
    for level in range(1, levels):
        count = group >> (level + 1)

        def later_copy(i):
            return pltpu.make_async_remote_copy(
                src_ref=later_out.at[slot + i],
                dst_ref=later_in.at[slot + i],
                send_sem=later_send.at[slot + i],
                recv_sem=later_recv.at[slot + i],
                device_id=depth_id(level),
                device_id_type=pl.DeviceIdType.MESH,
            )

        for i in range(count):
            away = 2 * i + 1 - bit(level)
            for channel in range(2):
                later_out[slot + i, channel] = encode(held[channel, away])
            later_copy(i).start()
        for i in range(count):
            stay = 2 * i + bit(level)
            later_copy(i).wait()
            keep = held[0, stay], held[1, stay]
            other = decode(later_in[slot + i, 0]), decode(later_in[slot + i, 1])
            held[0, i], held[1, i] = over(in_front(level), keep, other)
        slot += count

    color_out[...] = held[0, 0]
    alpha_out[...] = held[1, 0]


def shards(
    density, occupancy, shear_offsets, frac_lateral, frac_vertical, extinction, slab_gain, view_rank
):
    voxels = density[0]
    slices, rows, cols = voxels.shape
    row_blocks = rows // BLK
    group, lanes = lax.axis_size("depth"), lax.axis_size("lat")
    piece = rows // group
    pairs = BLK // (2 * piece)
    occ = occupancy[0].astype(jnp.float32)
    slice_total = group * slices
    prm = jnp.stack(
        [
            1.0 - frac_lateral[0],
            frac_lateral[0],
            2.0 * lax.reduce_precision(1.0 - frac_vertical[0], 8, 7),
            2.0 * lax.reduce_precision(frac_vertical[0], 8, 7),
            extinction[0] * (-0.5 * math.log2(math.e) / slice_total),
        ]
    )
    pad_rows = -row_blocks % 8
    occ_edge = jnp.broadcast_to(jnp.pad(occ[:, -1:], ((0, pad_rows), (0, 0))), (row_blocks + pad_rows, SHIFT))
    smem = pl.BlockSpec(memory_space=pltpu.SMEM)
    vmem = pl.BlockSpec(memory_space=pltpu.VMEM)
    later = group // 2 - 1
    dma = pltpu.SemaphoreType.DMA
    return pl.pallas_call(
        functools.partial(render_kernel, (slices, rows, cols, group, lanes)),
        in_specs=[pl.BlockSpec(memory_space=pl.ANY), vmem, smem, smem, smem, smem, smem],
        out_specs=[vmem, vmem],
        out_shape=[jax.ShapeDtypeStruct((piece, cols), jnp.float32)] * 2,
        scratch_shapes=[
            pltpu.VMEM((slices, rows, cols), jnp.bfloat16),
            pltpu.VMEM((slices, rows, SHIFT), jnp.bfloat16),
            pltpu.VMEM((row_blocks + pad_rows, SHIFT), jnp.float32),
            pltpu.VMEM((slices, 2 * SHIFT, SHIFT), jnp.bfloat16),
            pltpu.VMEM((2, group // 2, piece, cols), jnp.float32),
            pltpu.VMEM((row_blocks, 2, pairs, piece, cols), jnp.int16),
            pltpu.VMEM((row_blocks, 2, pairs, piece, cols), jnp.int16),
            pltpu.VMEM((later, 2, piece, cols), jnp.int16),
            pltpu.VMEM((later, 2, piece, cols), jnp.int16),
            dma((row_blocks,)),
            dma((row_blocks,)),
            dma((row_blocks,)),
            dma,
            dma,
            dma((row_blocks,)),
            dma((row_blocks,)),
            dma((later,)),
            dma((later,)),
        ],
        compiler_params=pltpu.CompilerParams(
            collective_id=0, has_side_effects=True, vmem_limit_bytes=48 * 2**20
        ),
    )(voxels, occ_edge, occ, shear_offsets, prm, slab_gain, view_rank)


def solution(mesh):
    placed = (
        P("depth", None, None, "lat"),
        P("depth", None, "lat"),
        P("depth", None),
        P("depth", None),
        P("depth", None),
        P("depth", None),
        P("depth"),
        P(),
    )
    return jax.shard_map(
        shards,
        mesh=mesh,
        in_specs=placed,
        out_specs=(P("depth", "lat"), P("depth", "lat")),
        check_vma=False,
    )
```

```python
import functools
import math

import jax
import jax.numpy as jnp
from jax import lax
from jax.experimental import pallas as pl
from jax.experimental.pallas import tpu as pltpu
from jax.sharding import PartitionSpec as P

SHIFT = 128
BLK = 128
HALO = 16


def rounded(x):
    return x.astype(jnp.bfloat16).astype(jnp.float32)


def build_weights(lmat, vertical, off, frac_lateral, frac_vertical, slices):
    source = lax.broadcasted_iota(jnp.int32, (2 * SHIFT, SHIFT), 0)
    target = lax.broadcasted_iota(jnp.int32, (2 * SHIFT, SHIFT), 1)
    lag = target + SHIFT - source
    for s in range(slices):
        part = frac_lateral[0, s]
        first = jnp.where(lag == off[0, s], 1.0 - part, 0.0)
        second = jnp.where(lag - 1 == off[0, s], part, 0.0)
        lmat[s] = (first + second).astype(jnp.bfloat16)
        down = frac_vertical[0, s]
        vertical[0, s] = 2.0 * rounded(jnp.full((HALO, SHIFT), 1.0 - down))
        vertical[1, s] = 2.0 * rounded(jnp.full((HALO, SHIFT), down))


def march(r, left, right, masks, lmat, vertical, extinction, scale, slices):
    row = pl.multiple_of(r * BLK, BLK)
    above = pl.multiple_of(jnp.maximum(r * BLK - HALO, 0), HALO)
    left_occ, left_halo, right_occ, right_halo = [
        jnp.broadcast_to(mask, (HALO, SHIFT)).astype(jnp.bfloat16) for mask in masks
    ]

    def scaled(read, s, start, count, by):
        return read(s, start, count) * jnp.concatenate([by] * (count // HALO), 0)

    through = jnp.ones((BLK, SHIFT), jnp.float32)
    color = jnp.zeros((BLK, SHIFT), jnp.float32)
    for s in range(slices):
        top = jnp.concatenate(
            [scaled(left, s, above, HALO, left_halo), scaled(right, s, above, HALO, right_halo)], 1
        )
        body = jnp.concatenate(
            [scaled(left, s, row, BLK, left_occ), scaled(right, s, row, BLK, right_occ)], 1
        )
        voxels = jnp.concatenate([top, body], 0)
        across = rounded(jnp.dot(voxels, lmat[s], preferred_element_type=jnp.float32))
        stay = jnp.concatenate([vertical[0, s]] * (BLK // HALO + 1), 0)
        fall = jnp.concatenate([vertical[1, s]] * (BLK // HALO + 1), 0)
        field = rounded(stay * across + fall * pltpu.roll(across, 1, 0))
        slope = (field - pltpu.roll(field, 1, 0))[HALO:]
        after = through * jnp.exp2((extinction[0, s] * scale) * field[HALO:])
        color = color + (through - after) * jnp.tanh(slope)
        through = after
    return color, through


def finish(color, through, gain):
    alpha = 1.0 - through
    return gain * (0.35 * color + 0.65 * alpha), alpha


def encode(x):
    return jnp.floor(x * 65535.0 - 32767.5).astype(jnp.int32).astype(jnp.int16)


def decode(x):
    return (x.astype(jnp.int32).astype(jnp.float32) + 32768.0) * (1.0 / 65535.0)


def over(in_front, keep, other):
    keep_color, keep_alpha = keep
    other_color, other_alpha = other
    front_color = jnp.where(in_front, keep_color, other_color)
    front_alpha = jnp.where(in_front, keep_alpha, other_alpha)
    back_color = jnp.where(in_front, other_color, keep_color)
    back_alpha = jnp.where(in_front, other_alpha, keep_alpha)
    return (
        front_color + (1.0 - front_alpha) * back_color,
        front_alpha + (1.0 - front_alpha) * back_alpha,
    )


def render_kernel(
    dims,
    density, occupancy_in, off_in, frac_lateral_in, frac_vertical_in, extinction_in, rank_in, gain,
    color_out, alpha_out,
    occupancy, off, frac_lateral, frac_vertical, extinction, view_rank,
    voxels, edge, occ_edge, occ_left, lmat, vertical, held, first_out, first_in, later_out, later_in,
    load_sem, edge_send, edge_recv, occ_send, occ_recv, first_send, first_recv,
    later_send, later_recv, small_sem,
):
    slices, rows, cols, group, lanes = dims
    row_blocks, col_blocks = rows // BLK, cols // SHIFT
    piece = rows // group
    pairs = BLK // (2 * piece)
    levels = group.bit_length() - 1
    early = pairs == 1 and levels > 1
    scale = -0.5 * math.log2(math.e) / (group * slices)
    me, lat = lax.axis_index("depth"), lax.axis_index("lat")
    has_left, has_right = lat > 0, lat < lanes - 1

    def depth_id(level):
        return {"depth": me ^ (1 << level), "lat": lat}

    def bit(level):
        return (me >> level) & 1

    def in_front(level):
        return ((view_rank[me] >> level) & 1) == 0

    small = [
        pltpu.make_async_copy(source, target, small_sem.at[k])
        for k, (source, target) in enumerate(
            [
                (occupancy_in, occupancy),
                (off_in, off),
                (frac_lateral_in, frac_lateral),
                (frac_vertical_in, frac_vertical),
                (extinction_in, extinction),
                (rank_in, view_rank),
            ]
        )
    ]
    for copy in small:
        copy.start()

    barrier = pltpu.get_barrier_semaphore()
    for level in range(levels):
        pl.semaphore_signal(
            barrier, inc=1, device_id=depth_id(level), device_id_type=pl.DeviceIdType.MESH
        )

    right_id = {"depth": me, "lat": jnp.minimum(lat + 1, lanes - 1)}
    left_id = {"depth": me, "lat": jnp.maximum(lat - 1, 0)}

    @pl.when(has_left)
    def _():
        pl.semaphore_signal(barrier, inc=1, device_id=left_id, device_id_type=pl.DeviceIdType.MESH)

    @pl.when(has_right)
    def _():
        pl.semaphore_signal(barrier, inc=1, device_id=right_id, device_id_type=pl.DeviceIdType.MESH)

    def load(r):
        span = pl.ds(pl.multiple_of(r * BLK, BLK), BLK)
        return pltpu.make_async_copy(
            density.at[:, span, :], voxels.at[:, span, :], load_sem.at[r]
        )

    def edge_copy(r):
        span = pl.ds(pl.multiple_of(r * BLK, BLK), BLK)
        return pltpu.make_async_remote_copy(
            src_ref=density.at[:, span, pl.ds(cols - SHIFT, SHIFT)],
            dst_ref=edge.at[:, span, :],
            send_sem=edge_send.at[r],
            recv_sem=edge_recv.at[r],
            device_id=right_id,
            device_id_type=pl.DeviceIdType.MESH,
        )

    occ_copy = pltpu.make_async_remote_copy(
        src_ref=occ_edge,
        dst_ref=occ_left,
        send_sem=occ_send,
        recv_sem=occ_recv,
        device_id=right_id,
        device_id_type=pl.DeviceIdType.MESH,
    )

    def first_copy(r):
        return pltpu.make_async_remote_copy(
            src_ref=first_out.at[r],
            dst_ref=first_in.at[r],
            send_sem=first_send.at[r],
            recv_sem=first_recv.at[r],
            device_id=depth_id(0),
            device_id_type=pl.DeviceIdType.MESH,
        )

    def occ(r, t):
        return occupancy[0, r, t].astype(jnp.float32)

    for r in range(row_blocks):
        load(r).start()

    for copy in small:
        copy.wait()

    occ_edge[...] = jnp.zeros_like(occ_edge)
    for r in range(row_blocks):
        occ_edge[pl.ds(r, 1), :] = jnp.full((1, SHIFT), occ(r, col_blocks - 1))

    @pl.when(jnp.logical_not(has_left))
    def _():
        edge[...] = jnp.zeros_like(edge)
        occ_left[...] = jnp.zeros_like(occ_left)

    build_weights(lmat, vertical, off, frac_lateral, frac_vertical, slices)

    wanted = levels + has_left.astype(jnp.int32) + has_right.astype(jnp.int32)
    pl.semaphore_wait(barrier, wanted)

    @pl.when(has_right)
    def _():
        occ_copy.start()
        for r in range(row_blocks):
            edge_copy(r).start()

    odd = bit(0) == 1
    zero = jnp.zeros((1, SHIFT), jnp.float32)

    def read_voxels(t):
        def read(s, start, count):
            return voxels[s, pl.ds(start, count), pl.ds(pl.multiple_of(t * SHIFT, SHIFT), SHIFT)]
        return read

    def read_edge(s, start, count):
        return edge[s, pl.ds(start, count), :]

    def tile(r, t, left, left_mask, left_halo):
        up = jnp.maximum(r - 1, 0)
        inside = jnp.where(r > 0, 1.0, 0.0)
        masks = (left_mask, left_halo * inside, zero + occ(r, t), zero + occ(up, t) * inside)
        result = finish(*march(r, left, read_voxels(t), masks, lmat, vertical, extinction, scale, slices), gain[0])
        lane = pl.ds(pl.multiple_of(t * SHIFT, SHIFT), SHIFT)
        for channel in range(2):
            for k in range(pairs):
                low = result[channel][2 * k * piece : (2 * k + 1) * piece]
                high = result[channel][(2 * k + 1) * piece : (2 * k + 2) * piece]
                held[channel, r * pairs + k, :, lane] = jnp.where(odd, high, low)
                first_out[r, channel, k, :, lane] = encode(jnp.where(odd, low, high))

    def first_merge(r):
        first_copy(r).wait()
        for k in range(pairs):
            keep = held[0, r * pairs + k], held[1, r * pairs + k]
            other = decode(first_in[r, 0, k]), decode(first_in[r, 1, k])
            held[0, r * pairs + k], held[1, r * pairs + k] = over(in_front(0), keep, other)

    def later_copy(level, slot):
        return pltpu.make_async_remote_copy(
            src_ref=later_out.at[slot],
            dst_ref=later_in.at[slot],
            send_sem=later_send.at[slot],
            recv_sem=later_recv.at[slot],
            device_id=depth_id(level),
            device_id_type=pl.DeviceIdType.MESH,
        )

    def later_start(level, slot, i):
        away = 2 * i + 1 - bit(level)
        for channel in range(2):
            later_out[slot, channel] = encode(held[channel, away])
        later_copy(level, slot).start()

    def row_step(r, carry):
        load(r).wait()

        def col_step(t, inner):
            up = jnp.maximum(r - 1, 0)
            tile(r, t, read_voxels(t - 1), zero + occ(r, t - 1), zero + occ(up, t - 1))
            return inner

        lax.fori_loop(1, col_blocks, col_step, 0)

        @pl.when(has_left & (r == 0))
        def _():
            occ_copy.wait_recv()

        @pl.when(has_left)
        def _():
            edge_copy(r).wait_recv()

        up = jnp.maximum(r - 1, 0)
        tile(r, 0, read_edge, occ_left[pl.ds(r, 1), :], occ_left[pl.ds(up, 1), :])
        first_copy(r).start()

        @pl.when(r > 0)
        def _():
            first_merge(r - 1)

        if early:

            @pl.when((r > 0) & (r % 2 == 0))
            def _():
                later_start(1, r // 2 - 1, r // 2 - 1)

        return carry

    lax.fori_loop(0, row_blocks, row_step, 0)

    @pl.when(has_right)
    def _():
        occ_copy.wait_send()
        for r in range(row_blocks):
            edge_copy(r).wait_send()

    first_merge(row_blocks - 1)

    slot = 0
    for level in range(1, levels):
        count = group >> (level + 1)
        for i in range(count):
            if not (early and level == 1 and i < count - 1):
                later_start(level, slot + i, i)
        for i in range(count):
            stay = 2 * i + bit(level)
            later_copy(level, slot + i).wait()
            keep = held[0, stay], held[1, stay]
            other = decode(later_in[slot + i, 0]), decode(later_in[slot + i, 1])
            held[0, i], held[1, i] = over(in_front(level), keep, other)
        slot += count

    color_out[...] = held[0, 0]
    alpha_out[...] = held[1, 0]


def shards(
    density, occupancy, shear_offsets, frac_lateral, frac_vertical, extinction, slab_gain, view_rank
):
    voxels = density[0]
    slices, rows, cols = voxels.shape
    row_blocks = rows // BLK
    group, lanes = lax.axis_size("depth"), lax.axis_size("lat")
    piece = rows // group
    pairs = BLK // (2 * piece)
    pad_rows = -row_blocks % 8
    hbm = pl.BlockSpec(memory_space=pltpu.HBM)
    small = (
        occupancy, shear_offsets, frac_lateral, frac_vertical, extinction, view_rank
    )
    vmem = pl.BlockSpec(memory_space=pltpu.VMEM)
    later = group // 2 - 1
    dma = pltpu.SemaphoreType.DMA
    return pl.pallas_call(
        functools.partial(render_kernel, (slices, rows, cols, group, lanes)),
        in_specs=[hbm] * 7 + [pl.BlockSpec(memory_space=pltpu.SMEM)],
        out_specs=[vmem, vmem],
        out_shape=[jax.ShapeDtypeStruct((piece, cols), jnp.float32)] * 2,
        scratch_shapes=[pltpu.SMEM(value.shape, value.dtype) for value in small]
        + [
            pltpu.VMEM((slices, rows, cols), jnp.bfloat16),
            pltpu.VMEM((slices, rows, SHIFT), jnp.bfloat16),
            pltpu.VMEM((row_blocks + pad_rows, SHIFT), jnp.float32),
            pltpu.VMEM((row_blocks + pad_rows, SHIFT), jnp.float32),
            pltpu.VMEM((slices, 2 * SHIFT, SHIFT), jnp.bfloat16),
            pltpu.VMEM((2, slices, HALO, SHIFT), jnp.float32),
            pltpu.VMEM((2, group // 2, piece, cols), jnp.float32),
            pltpu.VMEM((row_blocks, 2, pairs, piece, cols), jnp.int16),
            pltpu.VMEM((row_blocks, 2, pairs, piece, cols), jnp.int16),
            pltpu.VMEM((later, 2, piece, cols), jnp.int16),
            pltpu.VMEM((later, 2, piece, cols), jnp.int16),
            dma((row_blocks,)),
            dma((row_blocks,)),
            dma((row_blocks,)),
            dma,
            dma,
            dma((row_blocks,)),
            dma((row_blocks,)),
            dma((later,)),
            dma((later,)),
            dma((len(small),)),
        ],
        compiler_params=pltpu.CompilerParams(
            collective_id=0, has_side_effects=True, vmem_limit_bytes=67_043_328
        ),
    )(voxels, *small, slab_gain)


def solution(mesh):
    placed = (
        P("depth", None, None, "lat"),
        P("depth", None, "lat"),
        P("depth", None),
        P("depth", None),
        P("depth", None),
        P("depth", None),
        P("depth"),
        P(),
    )
    return jax.shard_map(
        shards,
        mesh=mesh,
        in_specs=placed,
        out_specs=(P("depth", "lat"), P("depth", "lat")),
        check_vma=False,
    )
```
